32 devices in a mesh: dp: 4 (over y, z), tp: 8 (over x, core).
Axes of the slice: x: 4, y: 2, z: 2, core: 2. Of those that a mesh axis runs over, the one named last changes fastest.
The devices are a block of a 4x4x8 slice.
Arguments:
- x_in: bfloat16 [8, 64, 4096], P('dp'), parts along dimension 0
- start_pos: int32 [8], P('dp'), parts along dimension 0
- kv_state: float32 [8, 16, 256, 512], P('dp', 'tp'), parts along dimension 0
- ln1_gain: float32 [4096], replicated
- ln1_bias: float32 [4096], replicated
- w_q: bfloat16 [4096, 4096], P(None, 'tp')
- w_k: bfloat16 [4096, 4096], P(None, 'tp')
- w_v: bfloat16 [4096, 8192], P(None, 'tp')
- w_g: bfloat16 [4096, 8192], P(None, 'tp')
- w_o: bfloat16 [8192, 4096], P('tp')
- ln2_gain: float32 [4096], replicated
- ln2_bias: float32 [4096], replicated
- w_up: bfloat16 [4096, 8192], P(None, 'tp')
- w_down: bfloat16 [8192, 4096], P('tp')
Outputs:
- output 1: bfloat16 [8, 64, 4096], P('dp'), parts along dimension 0
- output 2: float32 [8, 16, 256, 512], P('dp', 'tp'), parts along dimension 0
There are 4 independent parts. The reference program is written for one: setup_inputs(seed, part) draws one part's arguments, and reference() takes and returns one part's arrays. A program takes and returns all parts, laid end to end along the dimension named above; an argument that names none is the same for every part.
All inputs are finite; a program needn't handle non-finite values.
Results may differ from the reference program's by a relative error of at most 0.0145638.
Values are sent between devices in bfloat16 or wider.
A program may use at most 768 MiB of HBM per device.

```python
import jax
import jax.numpy as jnp
from jax import lax

BATCH_SEQS = 2
CHUNK_LEN = 64
D_MODEL = 4096
NUM_HEADS = 16
FFN_DIM = 8192
POS_LIMIT = 4096

KEY_DIM = D_MODEL // NUM_HEADS
VAL_DIM = 2 * KEY_DIM
HALF_DIM = KEY_DIM // 2
NORM_EPS = 1e-5
GROUP_EPS = 1e-6
ROPE_BASE = 10000.0


def head_log_decay():
    head_ids = jnp.arange(NUM_HEADS).astype(jnp.float32)
    return jnp.log1p(-jnp.exp2(-5.0 - head_ids))


def setup_inputs(seed: int = 0, part: int = 0) -> dict:
    base_key = jax.random.key(seed)
    weight_keys = jax.random.split(base_key, 12)
    part_keys = jax.random.split(jax.random.fold_in(weight_keys[11], part), 3)

    def normal_weight(key_index, arr_shape, fan_in):
        raw_draw = jax.random.normal(weight_keys[key_index], arr_shape, jnp.float32)
        return (raw_draw * fan_in ** -0.5).astype(jnp.bfloat16)

    x_in = jax.random.normal(part_keys[0], (BATCH_SEQS, CHUNK_LEN, D_MODEL), jnp.float32).astype(jnp.bfloat16)
    start_pos = jax.random.randint(part_keys[1], (BATCH_SEQS,), 64, POS_LIMIT, dtype=jnp.int32)
    log_gamma = head_log_decay()
    decayed_var = jnp.expm1(2.0 * start_pos.astype(jnp.float32)[:, None] * log_gamma[None, :]) / jnp.expm1(2.0 * log_gamma)[None, :]
    state_draw = jax.random.normal(part_keys[2], (BATCH_SEQS, NUM_HEADS, KEY_DIM, VAL_DIM), jnp.float32)
    kv_state = state_draw * jnp.sqrt(decayed_var / KEY_DIM)[:, :, None, None]
    return {
        'x_in': x_in,
        'start_pos': start_pos,
        'kv_state': kv_state,
        'ln1_gain': 1.0 + 0.3 * jax.random.normal(weight_keys[0], (D_MODEL,), jnp.float32),
        'ln1_bias': 0.3 * jax.random.normal(weight_keys[1], (D_MODEL,), jnp.float32),
        'w_q': normal_weight(2, (D_MODEL, D_MODEL), D_MODEL),
        'w_k': normal_weight(3, (D_MODEL, D_MODEL), D_MODEL),
        'w_v': normal_weight(4, (D_MODEL, 2 * D_MODEL), D_MODEL),
        'w_g': normal_weight(5, (D_MODEL, 2 * D_MODEL), D_MODEL),
        'w_o': normal_weight(6, (2 * D_MODEL, D_MODEL), 2 * D_MODEL),
        'ln2_gain': 1.0 + 0.3 * jax.random.normal(weight_keys[7], (D_MODEL,), jnp.float32),
        'ln2_bias': 0.3 * jax.random.normal(weight_keys[8], (D_MODEL,), jnp.float32),
        'w_up': normal_weight(9, (D_MODEL, FFN_DIM), D_MODEL),
        'w_down': normal_weight(10, (FFN_DIM, D_MODEL), FFN_DIM),
    }


def layer_norm(x_f32, norm_gain, norm_bias):
    row_mean = jnp.mean(x_f32, axis=-1, keepdims=True)
    centered = x_f32 - row_mean
    variance = jnp.mean(centered * centered, axis=-1, keepdims=True)
    return centered * lax.rsqrt(variance + NORM_EPS) * norm_gain + norm_bias


def rotate_half(head_vecs, cos_t, sin_t):
    first_half = head_vecs[..., :HALF_DIM]
    second_half = head_vecs[..., HALF_DIM:]
    return jnp.concatenate([first_half * cos_t - second_half * sin_t, second_half * cos_t + first_half * sin_t], axis=-1)


def reference(x_in, start_pos, kv_state, ln1_gain, ln1_bias, w_q, w_k, w_v, w_g, w_o, ln2_gain, ln2_bias, w_up, w_down):
    log_gamma = head_log_decay()
    step_ids = jnp.arange(CHUNK_LEN)
    step_gap = step_ids[:, None] - step_ids[None, :]
    inner_decay = jnp.where(step_gap[None] >= 0, jnp.exp(jnp.maximum(step_gap, 0).astype(jnp.float32)[None] * log_gamma[:, None, None]), 0.0)
    query_decay = jnp.exp((step_ids + 1).astype(jnp.float32)[:, None] * log_gamma[None, :])
    key_decay = jnp.exp((CHUNK_LEN - 1 - step_ids).astype(jnp.float32)[:, None] * log_gamma[None, :])
    state_decay = jnp.exp(CHUNK_LEN * log_gamma)
    inv_freq = jnp.power(ROPE_BASE, -jnp.arange(HALF_DIM).astype(jnp.float32) / HALF_DIM)

    def one_sequence(packed):
        tokens, first_pos, old_state = packed
        x_f32 = tokens.astype(jnp.float32)
        h_one = layer_norm(x_f32, ln1_gain, ln1_bias).astype(jnp.bfloat16)
        angles = (first_pos + step_ids).astype(jnp.float32)[:, None] * inv_freq[None, :]
        cos_t = jnp.cos(angles)[:, None, :]
        sin_t = jnp.sin(angles)[:, None, :]
        q_raw = jnp.dot(h_one, w_q, preferred_element_type=jnp.float32).reshape(CHUNK_LEN, NUM_HEADS, KEY_DIM)
        k_raw = jnp.dot(h_one, w_k, preferred_element_type=jnp.float32).reshape(CHUNK_LEN, NUM_HEADS, KEY_DIM)
        queries = rotate_half(q_raw, cos_t, sin_t).astype(jnp.bfloat16).astype(jnp.float32)
        keys = (rotate_half(k_raw, cos_t, sin_t) * KEY_DIM ** -0.5).astype(jnp.bfloat16).astype(jnp.float32)
        values = jnp.dot(h_one, w_v, preferred_element_type=jnp.float32).astype(jnp.bfloat16).astype(jnp.float32).reshape(CHUNK_LEN, NUM_HEADS, VAL_DIM)
        gates = jnp.dot(h_one, w_g, preferred_element_type=jnp.float32).reshape(CHUNK_LEN, NUM_HEADS, VAL_DIM)
        scores = jnp.einsum('chk,jhk->hcj', queries, keys) * inner_decay
        retained = jnp.einsum('hcj,jhe->che', scores, values) + jnp.einsum('chk,hke->che', queries, old_state) * query_decay[:, :, None]
        row_mean = jnp.mean(retained, axis=-1, keepdims=True)
        centered = retained - row_mean
        variance = jnp.mean(centered * centered, axis=-1, keepdims=True)
        normed = centered * lax.rsqrt(variance + GROUP_EPS)
        mixed = (jax.nn.silu(gates) * normed).astype(jnp.bfloat16).reshape(CHUNK_LEN, 2 * D_MODEL)
        attn_out = jnp.dot(mixed, w_o, preferred_element_type=jnp.float32).astype(jnp.bfloat16)
        x_mid = (x_f32 + attn_out.astype(jnp.float32)).astype(jnp.bfloat16)
        h_two = layer_norm(x_mid.astype(jnp.float32), ln2_gain, ln2_bias).astype(jnp.bfloat16)
        activated = jax.nn.gelu(jnp.dot(h_two, w_up, preferred_element_type=jnp.float32), approximate=False).astype(jnp.bfloat16)
        ffn_out = jnp.dot(activated, w_down, preferred_element_type=jnp.float32).astype(jnp.bfloat16)
        x_out = (x_mid.astype(jnp.float32) + ffn_out.astype(jnp.float32)).astype(jnp.bfloat16)
        new_state = state_decay[:, None, None] * old_state + jnp.einsum('jhk,jhe->hke', keys * key_decay[:, :, None], values)
        return x_out, new_state

    x_out, state_out = lax.map(one_sequence, (x_in, start_pos, kv_state))
    return (x_out, state_out)
```

```python
import functools

import jax
import jax.numpy as jnp
from jax import lax
from jax.experimental import pallas as pl
from jax.experimental.pallas import tpu as pltpu
from jax.sharding import PartitionSpec as P

NORM_EPS = 1e-5
GROUP_EPS = 1e-6
ROPE_BASE = 10000.0
NUM_CHUNKS = 4
MESH = pl.DeviceIdType.MESH
F32 = jnp.float32
BF16 = jnp.bfloat16


def layer_norm(x_f32, norm_gain, norm_bias):
    row_mean = jnp.mean(x_f32, axis=-1, keepdims=True)
    centered = x_f32 - row_mean
    variance = jnp.mean(centered * centered, axis=-1, keepdims=True)
    return centered * lax.rsqrt(variance + NORM_EPS) * norm_gain + norm_bias


def rotate_half(head_vecs, cos_t, sin_t):
    half_dim = head_vecs.shape[-1] // 2
    first_half = head_vecs[..., :half_dim]
    second_half = head_vecs[..., half_dim:]
    return jnp.concatenate([first_half * cos_t - second_half * sin_t, second_half * cos_t + first_half * sin_t], axis=-1)


def rope_tables(first_pos, chunk_len, key_dim):
    half_dim = key_dim // 2
    inv_freq = jnp.power(ROPE_BASE, -jnp.arange(half_dim).astype(jnp.float32) / half_dim)
    positions = (first_pos[:, None] + jnp.arange(chunk_len)[None, :]).astype(jnp.float32)
    angles = positions[:, :, None] * inv_freq
    return jnp.cos(angles)[:, :, None, :], jnp.sin(angles)[:, :, None, :]


def head_log_decay(head_ids):
    return jnp.log1p(-jnp.exp2(-5.0 - head_ids.astype(jnp.float32)))


def project_heads(h_one, cos_t, sin_t, w_q, w_k, w_v, w_g, num_heads):
    d_model = h_one.shape[-1]
    key_dim = w_q.shape[1] // num_heads
    val_dim = w_v.shape[1] // num_heads
    q_raw = jnp.einsum('bcd,dhk->bchk', h_one, w_q.reshape(d_model, num_heads, key_dim), preferred_element_type=jnp.float32)
    k_raw = jnp.einsum('bcd,dhk->bchk', h_one, w_k.reshape(d_model, num_heads, key_dim), preferred_element_type=jnp.float32)
    queries = rotate_half(q_raw, cos_t, sin_t).astype(jnp.bfloat16)
    keys = (rotate_half(k_raw, cos_t, sin_t) * key_dim ** -0.5).astype(jnp.bfloat16)
    values = jnp.einsum('bcd,dhe->bche', h_one, w_v.reshape(d_model, num_heads, val_dim), preferred_element_type=jnp.float32).astype(jnp.bfloat16)
    gates = jnp.einsum('bcd,dhe->bche', h_one, w_g.reshape(d_model, num_heads, val_dim), preferred_element_type=jnp.float32)
    return queries, keys, values, gates


def mix_heads(queries, keys, values_f32, gates, state_in, log_gamma):
    chunk_len = queries.shape[1]
    step_ids = jnp.arange(chunk_len)
    step_gap = step_ids[:, None] - step_ids[None, :]
    inner_decay = jnp.where(step_gap[None] >= 0, jnp.exp(jnp.maximum(step_gap, 0).astype(jnp.float32)[None] * log_gamma[:, None, None]), 0.0)
    query_decay = jnp.exp((step_ids + 1).astype(jnp.float32)[:, None] * log_gamma[None, :])
    scores = jnp.einsum('bchk,bjhk->bhcj', queries, keys, preferred_element_type=jnp.float32) * inner_decay
    retained = jnp.einsum('bhcj,bjhe->bche', scores, values_f32) + jnp.einsum('bchk,bhke->bche', queries.astype(jnp.float32), state_in) * query_decay[:, :, None]
    row_mean = jnp.mean(retained, axis=-1, keepdims=True)
    centered = retained - row_mean
    variance = jnp.mean(centered * centered, axis=-1, keepdims=True)
    normed = centered * lax.rsqrt(variance + GROUP_EPS)
    return (jax.nn.silu(gates) * normed).astype(jnp.bfloat16)


def chunk_state(keys, values_f32, log_gamma):
    chunk_len = keys.shape[1]
    step_ids = jnp.arange(chunk_len)
    key_decay = jnp.exp((chunk_len - 1 - step_ids).astype(jnp.float32)[:, None] * log_gamma[None, :])
    return jnp.einsum('bjhk,bjhe->bhke', keys.astype(jnp.float32) * key_decay[:, :, None], values_f32)


def tail_kernel(z_ref, x_hbm, wo_hbm, wu_hbm, wd_hbm, gain_ref, bias_ref, out_ref,
                wo, wu, wd, x_own, keep, act, h_all, x_mid,
                pair_tx, pair_rx, far_tx, far_rx, near_tx, near_rx,
                w_sem, x_sem,
                pair_ss, pair_rs, far_ss, far_rs, near_ss, near_rs,
                ag_ss, ag_rs, fw_ss, fw_rs, d2d_ss, d2d_rs):
    nc = NUM_CHUNKS
    rows, d_model = out_ref.shape
    width = d_model // nc
    half = width // 2
    cls_rows = rows // 2
    blk = cls_rows // 4
    me = lax.axis_index('tp')
    chip = lax.div(me, 2)
    core = lax.rem(me, 2)
    right = {'tp': lax.rem(chip + 1, 4) * 2 + core}
    left = {'tp': lax.rem(chip + 3, 4) * 2 + core}
    other = {'tp': chip * 2 + (1 - core)}
    own_cls = pl.multiple_of(core * cls_rows, cls_rows)
    oth_cls = pl.multiple_of((1 - core) * cls_rows, cls_rows)

    def blk_at(k):
        return pl.multiple_of(lax.rem(chip + k, 4) * blk, blk)

    b_own, b_right, b_far, b_left = blk_at(0), blk_at(1), blk_at(2), blk_at(3)

    def rdma(src, dst, ss, rs, dev):
        return pltpu.make_async_remote_copy(src_ref=src, dst_ref=dst, send_sem=ss, recv_sem=rs, device_id=dev, device_id_type=MESH)

    loads = {}
    for j in range(nc):
        cs = pl.ds(j * width, width)
        loads['o', j] = pltpu.make_async_copy(wo_hbm.at[:, cs], wo.at[:, cs], w_sem.at[0, j])
        loads['u', j] = pltpu.make_async_copy(wu_hbm.at[cs, :], wu.at[cs, :], w_sem.at[1, j])
        loads['d', j] = pltpu.make_async_copy(wd_hbm.at[:, cs], wd.at[:, cs], w_sem.at[2, j])
    x_load = pltpu.make_async_copy(x_hbm.at[pl.ds(own_cls + b_own, blk), :], x_own, x_sem)
    loads['o', 0].start()
    x_load.start()
    for j in range(1, nc):
        loads['o', j].start()
    for j in range(nc):
        loads['u', j].start()
    for j in range(nc):
        loads['d', j].start()

    barrier = pltpu.get_barrier_semaphore()
    for dev in (right, left, other):
        pl.semaphore_signal(barrier, inc=1, device_id=dev, device_id_type=MESH)
    pl.semaphore_wait(barrier, 3)

    sends = []

    def go(copy):
        copy.start()
        sends.append(copy)
        return copy

    def reduce_scatter(p, lhs_keep, lhs_send, w_ref, tag, finish):
        near = {}

        def compute(j):
            loads[tag, j].wait()
            cs = pl.ds(j * width, width)
            part = jnp.dot(jnp.concatenate([lhs_send(), lhs_keep()], axis=0), w_ref[:, cs], preferred_element_type=F32)
            pair_tx[p, :, cs] = part[:cls_rows].astype(BF16)
            keep[:, cs] = part[cls_rows:]
            go(rdma(pair_tx.at[p, :, cs], pair_rx.at[p, :, cs], pair_ss.at[p, j], pair_rs.at[p, j], other))

        def pair(j):
            cs = pl.ds(j * width, width)
            rdma(pair_tx.at[p, :, cs], pair_rx.at[p, :, cs], pair_ss.at[p, j], pair_rs.at[p, j], other).wait_recv()
            far = keep[pl.ds(b_far, blk), cs] + pair_rx[p, pl.ds(b_far, blk), cs].astype(F32)
            far_tx[p, :, cs] = far.astype(BF16)
            for s, dev in ((0, right), (1, left)):
                hs = pl.ds(j * width + s * half, half)
                go(rdma(far_tx.at[p, :, hs], far_rx.at[p, :, hs], far_ss.at[p, j, s], far_rs.at[p, j, s], dev))

        def relay(j):
            cs = pl.ds(j * width, width)
            for s, dev, blk_id in ((0, right, b_right), (1, left, b_left)):
                hs = pl.ds(j * width + s * half, half)
                os = pl.ds(j * width + (1 - s) * half, half)
                rdma(far_tx.at[p, :, hs], far_rx.at[p, :, hs], far_ss.at[p, j, s], far_rs.at[p, j, s], dev).wait_recv()
                bs = pl.ds(blk_id, blk)
                near_tx[p, s, :, hs] = (keep[bs, hs] + pair_rx[p, bs, hs].astype(F32) + far_rx[p, :, hs].astype(F32)).astype(BF16)
                near_tx[p, s, :, os] = (keep[bs, os] + pair_rx[p, bs, os].astype(F32)).astype(BF16)
                go(rdma(near_tx.at[p, s, :, cs], near_rx.at[p, s, :, cs], near_ss.at[p, j, s], near_rs.at[p, j, s], dev))

        def final(j):
            cs = pl.ds(j * width, width)
            bs = pl.ds(b_own, blk)
            total = keep[bs, cs] + pair_rx[p, bs, cs].astype(F32)
            for s, dev in ((0, right), (1, left)):
                rdma(near_tx.at[p, s, :, cs], near_rx.at[p, s, :, cs], near_ss.at[p, j, s], near_rs.at[p, j, s], dev).wait_recv()
                total = total + near_rx[p, s, :, cs].astype(F32)
            finish(j, total)

        for t in range(nc + 6):
            if t < nc:
                compute(t)
            if 0 <= t - 2 < nc:
                pair(t - 2)
            if 0 <= t - 4 < nc:
                relay(t - 4)
            if 0 <= t - 6 < nc:
                final(t - 6)

    def gather_send(p, buf, j):
        rs = pl.ds(own_cls + b_own, blk)
        cs = pl.ds(j * width, width)
        for s, dev in ((0, right), (1, left)):
            go(rdma(buf.at[rs, cs], buf.at[rs, cs], ag_ss.at[p, j, s], ag_rs.at[p, j, s], dev))
        go(rdma(buf.at[rs, cs], buf.at[rs, cs], d2d_ss.at[p, j, 0], d2d_rs.at[p, j, 0], other))

    def gather_forward(p, buf, j):
        cs = pl.ds(j * width, width)
        for s, dev, back, blk_id in ((0, right, left, b_left), (1, left, right, b_right)):
            rs = pl.ds(own_cls + blk_id, blk)
            hs = pl.ds(j * width + s * half, half)
            rdma(buf.at[rs, cs], buf.at[rs, cs], ag_ss.at[p, j, s], ag_rs.at[p, j, s], dev).wait_recv()
            go(rdma(buf.at[rs, hs], buf.at[rs, hs], fw_ss.at[p, j, s], fw_rs.at[p, j, s], dev))
            go(rdma(buf.at[rs, cs], buf.at[rs, cs], d2d_ss.at[p, j, 1 + s], d2d_rs.at[p, j, 1 + s], other))

    def gather_far(p, buf, j):
        cs = pl.ds(j * width, width)
        rs = pl.ds(own_cls + b_far, blk)
        for s, dev in ((0, right), (1, left)):
            hs = pl.ds(j * width + s * half, half)
            rdma(buf.at[rs, hs], buf.at[rs, hs], fw_ss.at[p, j, s], fw_rs.at[p, j, s], dev).wait_recv()
        go(rdma(buf.at[rs, cs], buf.at[rs, cs], d2d_ss.at[p, j, 3], d2d_rs.at[p, j, 3], other))

    def gather_wait(p, buf, j):
        cs = pl.ds(j * width, width)
        for k, blk_id in enumerate((b_own, b_left, b_right, b_far)):
            rs = pl.ds(oth_cls + blk_id, blk)
            rdma(buf.at[rs, cs], buf.at[rs, cs], d2d_ss.at[p, j, k], d2d_rs.at[p, j, k], other).wait_recv()

    x_load.wait()

    def finish_u(j, total):
        cs = pl.ds(j * width, width)
        x_mid[:, cs] = (x_own[:, cs].astype(F32) + total.astype(BF16).astype(F32)).astype(BF16)

    reduce_scatter(0, lambda: z_ref[pl.ds(own_cls, cls_rows), :], lambda: z_ref[pl.ds(oth_cls, cls_rows), :], wo, 'o', finish_u)

    x1 = x_mid[...].astype(F32)
    mean = jnp.mean(x1, axis=-1, keepdims=True)
    centered = x1 - mean
    var = jnp.mean(centered * centered, axis=-1, keepdims=True)
    h_own = (centered * lax.rsqrt(var + NORM_EPS) * gain_ref[...] + bias_ref[...]).astype(BF16)
    h_all[pl.ds(own_cls + b_own, blk), :] = h_own
    for j in range(nc):
        gather_send(0, h_all, j)

    up = None
    for j in range(nc):
        gather_forward(0, h_all, j)
        if j > 0:
            gather_far(0, h_all, j - 1)
    gather_far(0, h_all, nc - 1)
    for j in range(nc):
        gather_wait(0, h_all, j)
        loads['u', j].wait()
        cs = pl.ds(j * width, width)
        part = jnp.dot(h_all[:, cs], wu[cs, :], preferred_element_type=F32)
        up = part if up is None else up + part
    act[...] = (0.5 * up * (1.0 + lax.erf(up * (0.5 ** 0.5)))).astype(BF16)

    def finish_f(j, total):
        cs = pl.ds(j * width, width)
        x2 = x_mid[:, cs].astype(F32) + total.astype(BF16).astype(F32)
        out_ref[pl.ds(own_cls + b_own, blk), cs] = x2.astype(BF16)
        gather_send(1, out_ref, j)

    reduce_scatter(1, lambda: act[pl.ds(own_cls, cls_rows), :], lambda: act[pl.ds(oth_cls, cls_rows), :], wd, 'd', finish_f)
    for j in range(nc):
        gather_forward(1, out_ref, j)
        if j > 0:
            gather_far(1, out_ref, j - 1)
    gather_far(1, out_ref, nc - 1)
    for j in range(nc):
        gather_wait(1, out_ref, j)
    for copy in sends:
        copy.wait_send()


def tail(z, x2d, w_o, w_up, w_down, gain, bias):
    rows, d_model = x2d.shape
    inner = z.shape[1]
    ffn = w_up.shape[1]
    nc = NUM_CHUNKS
    blk = rows // 8
    dma = pltpu.SemaphoreType.DMA
    vmem = pl.BlockSpec(memory_space=pltpu.VMEM)
    hbm = pl.BlockSpec(memory_space=pl.ANY)
    return pl.pallas_call(
        tail_kernel,
        out_shape=jax.ShapeDtypeStruct((rows, d_model), BF16),
        in_specs=[vmem, hbm, hbm, hbm, hbm, vmem, vmem],
        out_specs=vmem,
        scratch_shapes=[
            pltpu.VMEM((inner, d_model), BF16),
            pltpu.VMEM((d_model, ffn), BF16),
            pltpu.VMEM((ffn, d_model), BF16),
            pltpu.VMEM((blk, d_model), BF16),
            pltpu.VMEM((rows // 2, d_model), F32),
            pltpu.VMEM((rows, ffn), BF16),
            pltpu.VMEM((rows, d_model), BF16),
            pltpu.VMEM((blk, d_model), BF16),
            pltpu.VMEM((2, rows // 2, d_model), BF16),
            pltpu.VMEM((2, rows // 2, d_model), BF16),
            pltpu.VMEM((2, blk, d_model), BF16),
            pltpu.VMEM((2, blk, d_model), BF16),
            pltpu.VMEM((2, 2, blk, d_model), BF16),
            pltpu.VMEM((2, 2, blk, d_model), BF16),
            dma((3, nc)),
            dma,
            dma((2, nc)), dma((2, nc)),
            dma((2, nc, 2)), dma((2, nc, 2)),
            dma((2, nc, 2)), dma((2, nc, 2)),
            dma((2, nc, 2)), dma((2, nc, 2)),
            dma((2, nc, 2)), dma((2, nc, 2)),
            dma((2, nc, 4)), dma((2, nc, 4)),
        ],
        compiler_params=pltpu.CompilerParams(collective_id=0, has_side_effects=True, vmem_limit_bytes=60 * 1024 * 1024),
        name='tail',
    )(z, x2d, w_o, w_up, w_down, gain, bias)


def solution(mesh):
    def local_layer(x_in, start_pos, kv_state, ln1_gain, ln1_bias, w_q, w_k, w_v, w_g, w_o, ln2_gain, ln2_bias, w_up, w_down):
        local_heads = kv_state.shape[1]
        batch, chunk_len, d_model = x_in.shape
        head_ids = lax.axis_index('tp') * local_heads + jnp.arange(local_heads)
        log_gamma = head_log_decay(head_ids)
        x_f32 = x_in.astype(jnp.float32)
        h_one = layer_norm(x_f32, ln1_gain, ln1_bias).astype(jnp.bfloat16)
        cos_t, sin_t = rope_tables(start_pos, chunk_len, kv_state.shape[2])
        queries, keys, values, gates = project_heads(h_one, cos_t, sin_t, w_q, w_k, w_v, w_g, local_heads)
        values_f32 = values.astype(jnp.float32)
        mixed = mix_heads(queries, keys, values_f32, gates, kv_state, log_gamma)
        new_state = jnp.exp(chunk_len * log_gamma)[:, None, None] * kv_state + chunk_state(keys, values_f32, log_gamma)
        rows = batch * chunk_len
        x_out = tail(mixed.reshape(rows, -1), x_in.reshape(rows, d_model), w_o, w_up, w_down, ln2_gain.reshape(1, -1), ln2_bias.reshape(1, -1))
        return x_out.reshape(x_in.shape), new_state

    in_specs = (P('dp', None, None), P('dp'), P('dp', 'tp', None, None), P(), P(), P(None, 'tp'), P(None, 'tp'), P(None, 'tp'), P(None, 'tp'), P('tp', None), P(), P(), P(None, 'tp'), P('tp', None))
    out_specs = (P('dp', None, None), P('dp', 'tp', None, None))
    return jax.shard_map(local_layer, mesh=mesh, in_specs=in_specs, out_specs=out_specs, check_vma=False)
```

```python
import jax
import jax.numpy as jnp
import numpy as np
from jax import lax
from jax.experimental import pallas as pl
from jax.experimental.pallas import tpu as pltpu
from jax.sharding import PartitionSpec as P

NORM_EPS = 1e-5
GROUP_EPS = 1e-6
ROPE_BASE = 10000.0
NUM_CHUNKS = 4
SCHEDULE = (
    [('compute', 0), ('compute', 1), ('compute', 2), ('pair', 0), ('compute', 3), ('pair', 1), ('pair', 2), ('pair', 3)]
    + [('relay', j) for j in range(NUM_CHUNKS)] + [('final', j) for j in range(NUM_CHUNKS)]
)
MESH = pl.DeviceIdType.MESH
F32 = jnp.float32
BF16 = jnp.bfloat16


def head_kernel(pos_ref, lg_ref, freq_ref, gain_ref, bias_ref, x_hbm, s_hbm, wq_hbm, wk_hbm, wv_hbm, wg_hbm, z_ref, s_out,
                x, h, wq, wk, wv, wg, s_in, s_new, q, k, v, o, sem, out_sem):
    batch, heads, key_dim, val_dim = s_hbm.shape
    rows, d_model = x.shape
    chunk = rows // batch
    half = key_dim // 2
    me = lax.axis_index('tp')

    loads = {}

    def add(name, src, dst):
        loads[name] = pltpu.make_async_copy(src, dst, sem.at[len(loads)])

    add('x', x_hbm, x)
    for name, src, dst, pieces in (('q', wq_hbm, wq, 2), ('k', wk_hbm, wk, 2), ('s', s_hbm, s_in, 1), ('v', wv_hbm, wv, 4), ('g', wg_hbm, wg, 4)):
        if pieces == 1:
            add((name, 0), src, dst)
        else:
            for i in range(pieces):
                rs = pl.ds(i * (d_model // pieces), d_model // pieces)
                add((name, i), src.at[rs, :], dst.at[rs, :])
    order = list(loads)
    state = {'next': 0}

    def issue(count):
        for name in order[state['next']:state['next'] + count]:
            loads[name].start()
        state['next'] += count

    def wait(name, count=1):
        with jax.named_scope('load'):
            loads[name].wait()
        issue(count)

    issue(5)

    with jax.named_scope('tables'):
        token = lax.broadcasted_iota(jnp.int32, (chunk, half), 0)
        pos = jnp.concatenate([token + pos_ref[b] for b in range(batch)], axis=0)
        angles = pos.astype(F32) * freq_ref[...]
        cos_t = jnp.cos(angles)
        sin_t = jnp.sin(angles)

    wait('x', 0)
    with jax.named_scope('ln1'):
        step = 16
        for r in range(0, rows, step):
            rs = pl.ds(r, step)
            xf = x[rs, :].astype(F32)
            mean = jnp.mean(xf, axis=-1, keepdims=True)
            centered = xf - mean
            var = jnp.mean(centered * centered, axis=-1, keepdims=True)
            h[rs, :] = (centered * lax.rsqrt(var + NORM_EPS) * gain_ref[...] + bias_ref[...]).astype(BF16)

    def project(name, w, pieces):
        total = None
        for i in range(pieces):
            wait((name, i))
            with jax.named_scope(f'dot_{name}{i}'):
                rs = pl.ds(i * (d_model // pieces), d_model // pieces)
                part = jnp.dot(h[:, rs], w[rs, :], preferred_element_type=F32)
                total = part if total is None else total + part
        return total

    def rotate(dst, raw, scale):
        for n in range(heads):
            a = raw[:, n * key_dim:n * key_dim + half]
            b = raw[:, n * key_dim + half:(n + 1) * key_dim]
            dst[:, pl.ds(n * key_dim, half)] = ((a * cos_t - b * sin_t) * scale).astype(BF16)
            dst[:, pl.ds(n * key_dim + half, half)] = ((b * cos_t + a * sin_t) * scale).astype(BF16)

    rotate(q, project('q', wq, 2), 1.0)
    rotate(k, project('k', wk, 2), key_dim ** -0.5)
    wait(('s', 0))
    v[...] = project('v', wv, 4).astype(BF16)

    row = lax.broadcasted_iota(jnp.int32, (chunk, chunk), 0)
    col = lax.broadcasted_iota(jnp.int32, (chunk, chunk), 1)
    gap = jnp.maximum(row - col, 0).astype(F32)
    nth = lax.broadcasted_iota(jnp.int32, (chunk, 1), 0).astype(F32)

    def split(a):
        hi = a.astype(BF16)
        return hi, (a - hi.astype(F32)).astype(BF16)

    outs = []
    for n in range(heads):
        log_gamma = lg_ref[me * heads + n]
        inner = jnp.where(row >= col, jnp.exp(gap * log_gamma), 0.0)
        q_decay = jnp.exp((nth + 1.0) * log_gamma)
        k_decay = jnp.exp((chunk - 1.0 - nth) * log_gamma)
        s_decay = jnp.exp(jnp.full((1, val_dim), float(chunk), F32) * log_gamma)
        for b in range(batch):
            with jax.named_scope(f'mix{n}{b}'):
                bs = pl.ds(b * chunk, chunk)
                qb = q[bs, pl.ds(n * key_dim, key_dim)]
                kb = k[bs, pl.ds(n * key_dim, key_dim)]
                vb = v[bs, pl.ds(n * val_dim, val_dim)]
                v2 = jnp.concatenate([vb, vb], axis=0)
                scores = lax.dot_general(qb, kb, (((1,), (1,)), ((), ())), preferred_element_type=F32) * inner
                s_old = s_in[b, n]
                s_hi, s_lo = split(s_old)
                cross = jnp.dot(qb, s_hi, preferred_element_type=F32) + jnp.dot(qb, s_lo, preferred_element_type=F32)
                ret = jnp.dot(jnp.concatenate(split(scores), axis=1), v2, preferred_element_type=F32) + cross * q_decay
                mean = jnp.mean(ret, axis=-1, keepdims=True)
                centered = ret - mean
                var = jnp.mean(centered * centered, axis=-1, keepdims=True)
                o[bs, pl.ds(n * val_dim, val_dim)] = centered * lax.rsqrt(var + GROUP_EPS)
                kd = jnp.concatenate(split(kb.astype(F32) * k_decay), axis=0)
                s_new[b, n] = s_old * s_decay + lax.dot_general(kd, v2, (((0,), (0,)), ((), ())), preferred_element_type=F32)
                out = pltpu.make_async_copy(s_new.at[b, n], s_out.at[b, n], out_sem.at[b, n])
                out.start()
                outs.append(out)

    gates = project('g', wg, 4)
    with jax.named_scope('gate'):
        z_ref[...] = (gates * jax.nn.sigmoid(gates) * o[...]).astype(BF16)
    for out in outs:
        out.wait()


def head(pos, log_gamma, freq, gain, bias, x2d, kv_state, w_q, w_k, w_v, w_g):
    rows, d_model = x2d.shape
    batch, heads, key_dim, val_dim = kv_state.shape
    dma = pltpu.SemaphoreType.DMA
    vmem = pl.BlockSpec(memory_space=pltpu.VMEM)
    smem = pl.BlockSpec(memory_space=pltpu.SMEM)
    hbm = pl.BlockSpec(memory_space=pl.ANY)
    return pl.pallas_call(
        head_kernel,
        out_shape=(jax.ShapeDtypeStruct((rows, heads * val_dim), BF16), jax.ShapeDtypeStruct(kv_state.shape, F32)),
        in_specs=[smem, smem, vmem, vmem, vmem] + [hbm] * 6,
        out_specs=(vmem, hbm),
        scratch_shapes=[
            pltpu.VMEM((rows, d_model), BF16),
            pltpu.VMEM((rows, d_model), BF16),
            pltpu.VMEM(w_q.shape, BF16),
            pltpu.VMEM(w_k.shape, BF16),
            pltpu.VMEM(w_v.shape, BF16),
            pltpu.VMEM(w_g.shape, BF16),
            pltpu.VMEM(kv_state.shape, F32),
            pltpu.VMEM(kv_state.shape, F32),
            pltpu.VMEM((rows, heads * key_dim), BF16),
            pltpu.VMEM((rows, heads * key_dim), BF16),
            pltpu.VMEM((rows, heads * val_dim), BF16),
            pltpu.VMEM((rows, heads * val_dim), F32),
            dma((16,)),
            dma((batch, heads)),
        ],
        compiler_params=pltpu.CompilerParams(vmem_limit_bytes=60 * 1024 * 1024),
        name='head',
    )(pos, log_gamma, freq, gain, bias, x2d, kv_state, w_q, w_k, w_v, w_g)


def tail_kernel(z_ref, x_hbm, wo_hbm, wu_hbm, wd_hbm, gain_ref, bias_ref, out_ref,
                wo, wu, wd, x_own, keep, act, h_all, x_mid,
                pair_tx, pair_rx, far_tx, far_rx, near_tx, near_rx,
                w_sem, x_sem,
                pair_ss, pair_rs, far_ss, far_rs, near_ss, near_rs,
                ag_ss, ag_rs, fw_ss, fw_rs, d2d_ss, d2d_rs):
    nc = NUM_CHUNKS
    rows, d_model = out_ref.shape
    width = d_model // nc
    half = width // 2
    cls_rows = rows // 2
    blk = cls_rows // 4
    me = lax.axis_index('tp')
    chip = lax.div(me, 2)
    core = lax.rem(me, 2)
    right = {'tp': lax.rem(chip + 1, 4) * 2 + core}
    left = {'tp': lax.rem(chip + 3, 4) * 2 + core}
    other = {'tp': chip * 2 + (1 - core)}
    own_cls = pl.multiple_of(core * cls_rows, cls_rows)
    oth_cls = pl.multiple_of((1 - core) * cls_rows, cls_rows)

    def blk_at(k):
        return pl.multiple_of(lax.rem(chip + k, 4) * blk, blk)

    b_own, b_right, b_far, b_left = blk_at(0), blk_at(1), blk_at(2), blk_at(3)

    def rdma(src, dst, ss, rs, dev):
        return pltpu.make_async_remote_copy(src_ref=src, dst_ref=dst, send_sem=ss, recv_sem=rs, device_id=dev, device_id_type=MESH)

    loads = {}
    for j in range(nc):
        cs = pl.ds(j * width, width)
        loads['o', j] = pltpu.make_async_copy(wo_hbm.at[:, cs], wo.at[:, cs], w_sem.at[0, j])
        loads['u', j] = pltpu.make_async_copy(wu_hbm.at[cs, :], wu.at[cs, :], w_sem.at[1, j])
        loads['d', j] = pltpu.make_async_copy(wd_hbm.at[:, cs], wd.at[:, cs], w_sem.at[2, j])
    x_load = pltpu.make_async_copy(x_hbm.at[pl.ds(own_cls + b_own, blk), :], x_own, x_sem)
    x_load.start()
    for j in range(nc):
        loads['o', j].start()

    barrier = pltpu.get_barrier_semaphore()
    for dev in (right, left, other):
        pl.semaphore_signal(barrier, inc=1, device_id=dev, device_id_type=MESH)
    with jax.named_scope('barrier'):
        pl.semaphore_wait(barrier, 3)

    sends = []

    def go(copy):
        copy.start()
        sends.append(copy)
        return copy

    def reduce_scatter(p, lhs_keep, lhs_send, w_ref, tag, finish):
        near = {}

        def compute(j):
            loads[tag, j].wait()
            if p == 0:
                loads['u', j].start()
            cs = pl.ds(j * width, width)
            part = jnp.dot(jnp.concatenate([lhs_send(), lhs_keep()], axis=0), w_ref[:, cs], preferred_element_type=F32)
            pair_tx[p, :, cs] = part[:cls_rows].astype(BF16)
            keep[:, cs] = part[cls_rows:]
            go(rdma(pair_tx.at[p, :, cs], pair_rx.at[p, :, cs], pair_ss.at[p, j], pair_rs.at[p, j], other))

        def pair(j):
            cs = pl.ds(j * width, width)
            rdma(pair_tx.at[p, :, cs], pair_rx.at[p, :, cs], pair_ss.at[p, j], pair_rs.at[p, j], other).wait_recv()
            far = keep[pl.ds(b_far, blk), cs] + pair_rx[p, pl.ds(b_far, blk), cs].astype(F32)
            far_tx[p, :, cs] = far.astype(BF16)
            for s, dev in ((0, right), (1, left)):
                hs = pl.ds(j * width + s * half, half)
                go(rdma(far_tx.at[p, :, hs], far_rx.at[p, :, hs], far_ss.at[p, j, s], far_rs.at[p, j, s], dev))
            for s, dev, blk_id in ((0, right, b_right), (1, left, b_left)):
                hs = pl.ds(j * width + (1 - s) * half, half)
                bs = pl.ds(blk_id, blk)
                near_tx[p, s, :, hs] = (keep[bs, hs] + pair_rx[p, bs, hs].astype(F32)).astype(BF16)
                go(rdma(near_tx.at[p, s, :, hs], near_rx.at[p, s, :, hs], near_ss.at[p, j, s, 0], near_rs.at[p, j, s, 0], dev))

        def relay(j):
            for s, dev, blk_id in ((0, right, b_right), (1, left, b_left)):
                hs = pl.ds(j * width + s * half, half)
                bs = pl.ds(blk_id, blk)
                rdma(far_tx.at[p, :, hs], far_rx.at[p, :, hs], far_ss.at[p, j, s], far_rs.at[p, j, s], dev).wait_recv()
                near_tx[p, s, :, hs] = (keep[bs, hs] + pair_rx[p, bs, hs].astype(F32) + far_rx[p, :, hs].astype(F32)).astype(BF16)
                go(rdma(near_tx.at[p, s, :, hs], near_rx.at[p, s, :, hs], near_ss.at[p, j, s, 1], near_rs.at[p, j, s, 1], dev))

        def final(j):
            cs = pl.ds(j * width, width)
            bs = pl.ds(b_own, blk)
            total = keep[bs, cs] + pair_rx[p, bs, cs].astype(F32)
            for s, dev in ((0, right), (1, left)):
                for i, off in ((0, (1 - s) * half), (1, s * half)):
                    hs = pl.ds(j * width + off, half)
                    rdma(near_tx.at[p, s, :, hs], near_rx.at[p, s, :, hs], near_ss.at[p, j, s, i], near_rs.at[p, j, s, i], dev).wait_recv()
                total = total + near_rx[p, s, :, cs].astype(F32)
            finish(j, total)

        for name, lag in SCHEDULE:
            with jax.named_scope(f'{name}{p}{lag}'):
                {'compute': compute, 'pair': pair, 'relay': relay, 'final': final}[name](lag)

    def gather_send(p, buf, js):
        rs = pl.ds(own_cls + b_own, blk)
        for i in (0, 1):
            for j in js:
                for s, dev in ((0, right), (1, left)):
                    hs = pl.ds(j * width + (s if i == 0 else 1 - s) * half, half)
                    go(rdma(buf.at[rs, hs], buf.at[rs, hs], ag_ss.at[p, j, s, i], ag_rs.at[p, j, s, i], dev))
        for j in js:
            cs = pl.ds(j * width, width)
            go(rdma(buf.at[rs, cs], buf.at[rs, cs], d2d_ss.at[p, j, 0], d2d_rs.at[p, j, 0], other))

    def gather_forward(p, buf, j):
        for s, dev, blk_id in ((0, right, b_left), (1, left, b_right)):
            rs = pl.ds(own_cls + blk_id, blk)
            hs = pl.ds(j * width + s * half, half)
            rdma(buf.at[rs, hs], buf.at[rs, hs], ag_ss.at[p, j, s, 0], ag_rs.at[p, j, s, 0], dev).wait_recv()
            go(rdma(buf.at[rs, hs], buf.at[rs, hs], fw_ss.at[p, j, s], fw_rs.at[p, j, s], dev))

    def gather_cross(p, buf, j):
        cs = pl.ds(j * width, width)
        for s, dev, blk_id in ((0, right, b_left), (1, left, b_right)):
            rs = pl.ds(own_cls + blk_id, blk)
            hs = pl.ds(j * width + (1 - s) * half, half)
            rdma(buf.at[rs, hs], buf.at[rs, hs], ag_ss.at[p, j, s, 1], ag_rs.at[p, j, s, 1], dev).wait_recv()
            go(rdma(buf.at[rs, cs], buf.at[rs, cs], d2d_ss.at[p, j, 1 + s], d2d_rs.at[p, j, 1 + s], other))

    def gather_far(p, buf, j):
        cs = pl.ds(j * width, width)
        rs = pl.ds(own_cls + b_far, blk)
        for s, dev in ((0, right), (1, left)):
            hs = pl.ds(j * width + s * half, half)
            rdma(buf.at[rs, hs], buf.at[rs, hs], fw_ss.at[p, j, s], fw_rs.at[p, j, s], dev).wait_recv()
        go(rdma(buf.at[rs, cs], buf.at[rs, cs], d2d_ss.at[p, j, 3], d2d_rs.at[p, j, 3], other))

    def gather_wait(p, buf, j):
        cs = pl.ds(j * width, width)
        for k, blk_id in enumerate((b_own, b_left, b_right, b_far)):
            rs = pl.ds(oth_cls + blk_id, blk)
            rdma(buf.at[rs, cs], buf.at[rs, cs], d2d_ss.at[p, j, k], d2d_rs.at[p, j, k], other).wait_recv()

    x_load.wait()

    def finish_u(j, total):
        cs = pl.ds(j * width, width)
        x_mid[:, cs] = (x_own[:, cs].astype(F32) + total.astype(BF16).astype(F32)).astype(BF16)

    reduce_scatter(0, lambda: z_ref[pl.ds(own_cls, cls_rows), :], lambda: z_ref[pl.ds(oth_cls, cls_rows), :], wo, 'o', finish_u)

    with jax.named_scope('ln2'):
        x1 = x_mid[...].astype(F32)
        mean = jnp.mean(x1, axis=-1, keepdims=True)
        centered = x1 - mean
        var = jnp.mean(centered * centered, axis=-1, keepdims=True)
        h_own = (centered * lax.rsqrt(var + NORM_EPS) * gain_ref[...] + bias_ref[...]).astype(BF16)
        h_all[pl.ds(own_cls + b_own, blk), :] = h_own
    gather_send(0, h_all, range(nc))
    for j in range(nc):
        loads['d', j].start()

    up = None
    for name, stage in (('gforward', gather_forward), ('gcross', gather_cross), ('gfar', gather_far)):
        for j in range(nc):
            with jax.named_scope(f'{name}0{j}'):
                stage(0, h_all, j)
    for j in range(nc):
        with jax.named_scope(f'gwait0{j}'):
            gather_wait(0, h_all, j)
        with jax.named_scope(f'up{j}'):
            loads['u', j].wait()
            cs = pl.ds(j * width, width)
            part = jnp.dot(h_all[:, cs], wu[cs, :], preferred_element_type=F32)
            up = part if up is None else up + part
    with jax.named_scope('gelu'):
        act[...] = (0.5 * up * (1.0 + lax.erf(up * (0.5 ** 0.5)))).astype(BF16)

    def finish_f(j, total):
        cs = pl.ds(j * width, width)
        x2 = x_mid[:, cs].astype(F32) + total.astype(BF16).astype(F32)
        out_ref[pl.ds(own_cls + b_own, blk), cs] = x2.astype(BF16)
        gather_send(1, out_ref, [j])

    reduce_scatter(1, lambda: act[pl.ds(own_cls, cls_rows), :], lambda: act[pl.ds(oth_cls, cls_rows), :], wd, 'd', finish_f)
    for name, stage in (('gforward', gather_forward), ('gcross', gather_cross), ('gfar', gather_far)):
        for j in range(nc):
            with jax.named_scope(f'{name}1{j}'):
                stage(1, out_ref, j)
    for j in range(nc):
        with jax.named_scope(f'gwait1{j}'):
            gather_wait(1, out_ref, j)
    with jax.named_scope('drain'):
        for copy in sends:
            copy.wait_send()


def tail(z, x2d, w_o, w_up, w_down, gain, bias):
    rows, d_model = x2d.shape
    inner = z.shape[1]
    ffn = w_up.shape[1]
    nc = NUM_CHUNKS
    blk = rows // 8
    dma = pltpu.SemaphoreType.DMA
    vmem = pl.BlockSpec(memory_space=pltpu.VMEM)
    hbm = pl.BlockSpec(memory_space=pl.ANY)
    return pl.pallas_call(
        tail_kernel,
        out_shape=jax.ShapeDtypeStruct((rows, d_model), BF16),
        in_specs=[vmem, hbm, hbm, hbm, hbm, vmem, vmem],
        out_specs=vmem,
        scratch_shapes=[
            pltpu.VMEM((inner, d_model), BF16),
            pltpu.VMEM((d_model, ffn), BF16),
            pltpu.VMEM((ffn, d_model), BF16),
            pltpu.VMEM((blk, d_model), BF16),
            pltpu.VMEM((rows // 2, d_model), F32),
            pltpu.VMEM((rows, ffn), BF16),
            pltpu.VMEM((rows, d_model), BF16),
            pltpu.VMEM((blk, d_model), BF16),
            pltpu.VMEM((2, rows // 2, d_model), BF16),
            pltpu.VMEM((2, rows // 2, d_model), BF16),
            pltpu.VMEM((2, blk, d_model), BF16),
            pltpu.VMEM((2, blk, d_model), BF16),
            pltpu.VMEM((2, 2, blk, d_model), BF16),
            pltpu.VMEM((2, 2, blk, d_model), BF16),
            dma((3, nc)),
            dma,
            dma((2, nc)), dma((2, nc)),
            dma((2, nc, 2)), dma((2, nc, 2)),
            dma((2, nc, 2, 2)), dma((2, nc, 2, 2)),
            dma((2, nc, 2, 2)), dma((2, nc, 2, 2)),
            dma((2, nc, 2)), dma((2, nc, 2)),
            dma((2, nc, 4)), dma((2, nc, 4)),
        ],
        compiler_params=pltpu.CompilerParams(collective_id=0, has_side_effects=True, vmem_limit_bytes=60 * 1024 * 1024),
        name='tail',
    )(z, x2d, w_o, w_up, w_down, gain, bias)


def solution(mesh):
    n_tp = mesh.shape['tp']

    def local_layer(x_in, start_pos, kv_state, ln1_gain, ln1_bias, w_q, w_k, w_v, w_g, w_o, ln2_gain, ln2_bias, w_up, w_down):
        batch, chunk_len, d_model = x_in.shape
        _, local_heads, key_dim, _ = kv_state.shape
        x2d = x_in.reshape(batch * chunk_len, d_model)
        log_gamma = np.log1p(-np.exp2(-5.0 - np.arange(local_heads * n_tp))).astype(np.float32)
        freq = np.power(ROPE_BASE, -np.arange(key_dim // 2) / (key_dim // 2)).astype(np.float32).reshape(1, -1)
        mixed, new_state = head(start_pos, jnp.asarray(log_gamma), jnp.asarray(freq), ln1_gain.reshape(1, -1), ln1_bias.reshape(1, -1),
                                x2d, kv_state, w_q, w_k, w_v, w_g)
        x_out = tail(mixed, x2d, w_o, w_up, w_down, ln2_gain.reshape(1, -1), ln2_bias.reshape(1, -1))
        return x_out.reshape(x_in.shape), new_state

    in_specs = (P('dp', None, None), P('dp'), P('dp', 'tp', None, None), P(), P(), P(None, 'tp'), P(None, 'tp'), P(None, 'tp'), P(None, 'tp'), P('tp', None), P(), P(), P(None, 'tp'), P('tp', None))
    out_specs = (P('dp', None, None), P('dp', 'tp', None, None))
    return jax.shard_map(local_layer, mesh=mesh, in_specs=in_specs, out_specs=out_specs, check_vma=False)
```
